32 devices in a mesh: dp: 2 (over x), tp: 4 (over z), ep: 4 (over y, core).
Axes of the slice: x: 2, y: 2, z: 4, core: 2. Of those that a mesh axis runs over, the one named last changes fastest.
Arguments:
- hidden: bfloat16 [1024, 768], P(('dp', 'ep')), parts along dimension 0
- write_pos: int32 [1024], P(('dp', 'ep')), parts along dimension 0
- enc_mask: int32 [1024, 128], P(('dp', 'ep')), parts along dimension 0
- expert_idx: int32 [1024], P(('dp', 'ep')), parts along dimension 0
- self_keys: bfloat16 [2, 1024, 12, 32, 64], P(None, ('dp', 'ep'), 'tp'), parts along dimension 1
- self_values: bfloat16 [2, 1024, 12, 32, 64], P(None, ('dp', 'ep'), 'tp'), parts along dimension 1
- cross_keys: bfloat16 [2, 1024, 12, 128, 64], P(None, ('dp', 'ep'), 'tp'), parts along dimension 1
- cross_values: bfloat16 [2, 1024, 12, 128, 64], P(None, ('dp', 'ep'), 'tp'), parts along dimension 1
- rel_bias: float32 [12, 32], P('tp')
- norm_scale: float32 [2, 3, 768], replicated
- w_query: bfloat16 [2, 768, 768], P(None, None, 'tp')
- w_key: bfloat16 [2, 768, 768], P(None, None, 'tp')
- w_value: bfloat16 [2, 768, 768], P(None, None, 'tp')
- w_out: bfloat16 [2, 768, 768], P(None, 'tp')
- w_cross_query: bfloat16 [2, 768, 768], P(None, None, 'tp')
- w_cross_out: bfloat16 [2, 768, 768], P(None, 'tp')
- dense_gate: bfloat16 [768, 3072], P(None, 'tp')
- dense_up: bfloat16 [768, 3072], P(None, 'tp')
- dense_down: bfloat16 [3072, 768], P('tp')
- router: float32 [768, 8], replicated
- exp_gate: bfloat16 [8, 768, 3072], P('ep', None, 'tp')
- exp_up: bfloat16 [8, 768, 3072], P('ep', None, 'tp')
- exp_down: bfloat16 [8, 3072, 768], P('ep', 'tp')
Outputs:
- output 1: bfloat16 [1024, 768], P(('dp', 'ep')), parts along dimension 0
- output 2: bfloat16 [2, 1024, 12, 32, 64], P(None, ('dp', 'ep'), 'tp'), parts along dimension 1
- output 3: bfloat16 [2, 1024, 12, 32, 64], P(None, ('dp', 'ep'), 'tp'), parts along dimension 1
There are 2 independent parts. The reference program is written for one: setup_inputs(seed, part) draws one part's arguments, and reference() takes and returns one part's arrays. A program takes and returns all parts, laid end to end along the dimension named above; an argument that names none is the same for every part.
All inputs are finite; a program needn't handle non-finite values.
Results may differ from the reference program's by a relative error of at most 0.02.
Values are sent between devices in bfloat16 or wider.
A program may use at most 1 GiB of HBM per device.

```python
import jax
import jax.numpy as jnp
from jax import lax

D = 768
HEADS = 12
HEAD = 64
FF = 3072
EXPERTS = 8
TOK_DEV = 128
GROUPS = 4
CACHE = 32
SRC = 128
TOKENS = TOK_DEV * GROUPS
WIDTH = HEADS * HEAD
CAPACITY = (2 * TOK_DEV + EXPERTS - 1) // EXPERTS
EPS = 1e-6
NEG_BIG = -1e9


def setup_inputs(seed: int = 0, part: int = 0) -> dict:
    root = jax.random.key(seed)
    shared_root, part_root = jax.random.split(root)
    local = jax.random.fold_in(part_root, part)
    local_keys = jax.random.split(local, 10)
    shared_keys = jax.random.split(shared_root, 16)

    def normal(key, shape, scale):
        return jax.random.normal(key, shape, jnp.float32) * scale

    row_ids = jnp.arange(TOKENS)
    hidden = normal(local_keys[0], (TOKENS, D), 1.0).astype(jnp.bfloat16)
    pos_draw = jax.random.randint(local_keys[1], (TOKENS,), 0, CACHE)
    write_pos = jnp.where(row_ids == 0, CACHE - 1, pos_draw).astype(jnp.int32)
    src_len = jax.random.randint(local_keys[2], (TOKENS,), max(SRC // 4, 1), SRC + 1)
    src_len = jnp.where(row_ids == 1, SRC, src_len)
    enc_mask = (jnp.arange(SRC)[None, :] < src_len[:, None]).astype(jnp.int32)
    spread = jax.random.permutation(local_keys[3], TOKENS) % EXPERTS
    hot_expert = jax.random.randint(local_keys[4], (), 0, EXPERTS)
    to_hot = jax.random.randint(local_keys[5], (TOKENS,), 0, 4) == 0
    expert_idx = jnp.where(to_hot, hot_expert, spread).astype(jnp.int32)
    self_shape = (2, TOKENS, HEADS, CACHE, HEAD)
    cross_shape = (2, TOKENS, HEADS, SRC, HEAD)
    return {
        'hidden': hidden,
        'write_pos': write_pos,
        'enc_mask': enc_mask,
        'expert_idx': expert_idx,
        'self_keys': normal(local_keys[6], self_shape, 1.0).astype(jnp.bfloat16),
        'self_values': normal(local_keys[7], self_shape, 1.0).astype(jnp.bfloat16),
        'cross_keys': normal(local_keys[8], cross_shape, 1.0).astype(jnp.bfloat16),
        'cross_values': normal(local_keys[9], cross_shape, 1.0).astype(jnp.bfloat16),
        'rel_bias': normal(shared_keys[0], (HEADS, CACHE), 1.0),
        'norm_scale': jax.random.uniform(shared_keys[1], (2, 3, D), jnp.float32, 0.5, 1.5),
        'w_query': normal(shared_keys[2], (2, D, WIDTH), 2.0 * (D * HEAD) ** -0.5).astype(jnp.bfloat16),
        'w_key': normal(shared_keys[3], (2, D, WIDTH), D ** -0.5).astype(jnp.bfloat16),
        'w_value': normal(shared_keys[4], (2, D, WIDTH), D ** -0.5).astype(jnp.bfloat16),
        'w_out': normal(shared_keys[5], (2, WIDTH, D), WIDTH ** -0.5).astype(jnp.bfloat16),
        'w_cross_query': normal(shared_keys[6], (2, D, WIDTH), 2.0 * (D * HEAD) ** -0.5).astype(jnp.bfloat16),
        'w_cross_out': normal(shared_keys[7], (2, WIDTH, D), WIDTH ** -0.5).astype(jnp.bfloat16),
        'dense_gate': normal(shared_keys[8], (D, FF), D ** -0.5).astype(jnp.bfloat16),
        'dense_up': normal(shared_keys[9], (D, FF), D ** -0.5).astype(jnp.bfloat16),
        'dense_down': normal(shared_keys[10], (FF, D), FF ** -0.5).astype(jnp.bfloat16),
        'router': normal(shared_keys[11], (D, EXPERTS), 2.0 * D ** -0.5),
        'exp_gate': normal(shared_keys[12], (EXPERTS, D, FF), D ** -0.5).astype(jnp.bfloat16),
        'exp_up': normal(shared_keys[13], (EXPERTS, D, FF), D ** -0.5).astype(jnp.bfloat16),
        'exp_down': normal(shared_keys[14], (EXPERTS, FF, D), 0.5 * (EXPERTS / FF) ** 0.5).astype(jnp.bfloat16),
    }


def rms_norm(h_cur, scale):
    h_float = h_cur.astype(jnp.float32)
    inv_rms = lax.rsqrt(jnp.mean(h_float * h_float, axis=-1, keepdims=True) + EPS)
    return (h_float * inv_rms * scale).astype(jnp.bfloat16)


def add_residual(h_cur, delta):
    return (h_cur.astype(jnp.float32) + delta.astype(jnp.float32)).astype(jnp.bfloat16)


def project(normed, weight):
    return jnp.dot(normed, weight, preferred_element_type=jnp.float32)


def self_attention(normed, write_pos, keys, values, w_query, w_key, w_value, w_out, rel_bias):
    tokens = normed.shape[0]
    query = project(normed, w_query).astype(jnp.bfloat16).reshape(tokens, HEADS, HEAD)
    key_new = project(normed, w_key).astype(jnp.bfloat16).reshape(tokens, HEADS, HEAD)
    value_new = project(normed, w_value).astype(jnp.bfloat16).reshape(tokens, HEADS, HEAD)
    distance = write_pos[:, None] - jnp.arange(CACHE)[None, :]
    at_slot = (distance == 0)[:, None, :, None]
    keys = jnp.where(at_slot, key_new[:, :, None, :], keys)
    values = jnp.where(at_slot, value_new[:, :, None, :], values)
    scores = jnp.einsum('thd,thld->thl', query.astype(jnp.float32), keys.astype(jnp.float32))
    bias = jnp.take(rel_bias, jnp.maximum(distance, 0), axis=1)
    scores = jnp.where((distance >= 0)[:, None, :], scores + jnp.swapaxes(bias, 0, 1), NEG_BIG)
    attn_prob = jax.nn.softmax(scores, axis=-1).astype(jnp.bfloat16)
    context = jnp.einsum('thl,thld->thd', attn_prob.astype(jnp.float32), values.astype(jnp.float32)).astype(jnp.bfloat16)
    attn_out = project(context.reshape(tokens, WIDTH), w_out).astype(jnp.bfloat16)
    return attn_out, keys, values


def cross_attention(normed, enc_mask, keys, values, w_query, w_out):
    tokens = normed.shape[0]
    query = project(normed, w_query).astype(jnp.bfloat16).reshape(tokens, HEADS, HEAD)
    scores = jnp.einsum('thd,thsd->ths', query.astype(jnp.float32), keys.astype(jnp.float32))
    scores = jnp.where((enc_mask > 0)[:, None, :], scores, NEG_BIG)
    attn_prob = jax.nn.softmax(scores, axis=-1).astype(jnp.bfloat16)
    context = jnp.einsum('ths,thsd->thd', attn_prob.astype(jnp.float32), values.astype(jnp.float32)).astype(jnp.bfloat16)
    return project(context.reshape(tokens, WIDTH), w_out).astype(jnp.bfloat16)


def gated_ffn(normed, w_gate, w_up, w_down):
    product = (jax.nn.gelu(project(normed, w_gate)) * project(normed, w_up)).astype(jnp.bfloat16)
    return project(product, w_down).astype(jnp.bfloat16)


def switch_ffn(normed, expert_idx, router, exp_gate, exp_up, exp_down):
    logits = jnp.dot(normed.astype(jnp.float32), router)
    route_prob = jax.nn.softmax(logits, axis=-1)
    gate = jnp.take_along_axis(route_prob, expert_idx[:, None], axis=1)[:, 0]
    onehot = (expert_idx[:, None] == jnp.arange(EXPERTS)[None, :]).astype(jnp.int32)
    onehot = onehot.reshape(GROUPS, TOK_DEV, EXPERTS)
    slot = jnp.sum((jnp.cumsum(onehot, axis=1) - onehot) * onehot, axis=2)
    dispatch = (onehot[..., None] * (slot[:, :, None, None] == jnp.arange(CAPACITY))).astype(jnp.float32)
    x_groups = normed.reshape(GROUPS, TOK_DEV, D).astype(jnp.float32)
    buffers = jnp.einsum('gtec,gtd->egcd', dispatch, x_groups).astype(jnp.bfloat16)
    buffers = buffers.reshape(EXPERTS, GROUPS * CAPACITY, D)

    def run_expert(expert):
        rows, w_gate, w_up, w_down = expert
        return gated_ffn(rows, w_gate, w_up, w_down)

    expert_out = lax.map(run_expert, (buffers, exp_gate, exp_up, exp_down))
    expert_out = expert_out.reshape(EXPERTS, GROUPS, CAPACITY, D).astype(jnp.float32)
    combined = jnp.einsum('gtec,egcd->gtd', dispatch, expert_out).reshape(TOKENS, D)
    return gate[:, None] * combined


def attention_block(layer, h_cur, write_pos, enc_mask, self_keys, self_values, cross_keys, cross_values, rel_bias, norm_scale, w_query, w_key, w_value, w_out, w_cross_query, w_cross_out):
    def one_group(group):
        h_grp, pos_grp, mask_grp, keys_grp, values_grp, ckeys_grp, cvalues_grp = group
        normed = rms_norm(h_grp, norm_scale[layer, 0])
        attn_out, keys_grp, values_grp = self_attention(normed, pos_grp, keys_grp, values_grp, w_query[layer], w_key[layer], w_value[layer], w_out[layer], rel_bias)
        h_grp = add_residual(h_grp, attn_out)
        normed = rms_norm(h_grp, norm_scale[layer, 1])
        cross_out = cross_attention(normed, mask_grp, ckeys_grp, cvalues_grp, w_cross_query[layer], w_cross_out[layer])
        return add_residual(h_grp, cross_out), keys_grp, values_grp

    def grouped(array_in):
        return array_in.reshape((GROUPS, TOK_DEV) + array_in.shape[1:])

    h_grp, keys_new, values_new = lax.map(one_group, (grouped(h_cur), grouped(write_pos), grouped(enc_mask), grouped(self_keys[layer]), grouped(self_values[layer]), grouped(cross_keys[layer]), grouped(cross_values[layer])))
    return h_grp.reshape(TOKENS, D), keys_new.reshape(self_keys.shape[1:]), values_new.reshape(self_values.shape[1:])


def reference(hidden, write_pos, enc_mask, expert_idx, self_keys, self_values, cross_keys, cross_values, rel_bias, norm_scale, w_query, w_key, w_value, w_out, w_cross_query, w_cross_out, dense_gate, dense_up, dense_down, router, exp_gate, exp_up, exp_down):
    h_cur, keys_a, values_a = attention_block(0, hidden, write_pos, enc_mask, self_keys, self_values, cross_keys, cross_values, rel_bias, norm_scale, w_query, w_key, w_value, w_out, w_cross_query, w_cross_out)
    normed = rms_norm(h_cur, norm_scale[0, 2])
    h_cur = add_residual(h_cur, gated_ffn(normed, dense_gate, dense_up, dense_down))
    h_cur, keys_b, values_b = attention_block(1, h_cur, write_pos, enc_mask, self_keys, self_values, cross_keys, cross_values, rel_bias, norm_scale, w_query, w_key, w_value, w_out, w_cross_query, w_cross_out)
    normed = rms_norm(h_cur, norm_scale[1, 2])
    h_cur = add_residual(h_cur, switch_ffn(normed, expert_idx, router, exp_gate, exp_up, exp_down))
    return h_cur, jnp.stack([keys_a, keys_b]), jnp.stack([values_a, values_b])
```

```python
import functools

import jax
import jax.numpy as jnp
from jax import lax
from jax.experimental import pallas as pl
from jax.experimental.pallas import tpu as pltpu
from jax.sharding import PartitionSpec as P

EPS = 1e-6
NEG_BIG = -1e9
F32 = jnp.float32
BF16 = jnp.bfloat16
MESH = pl.DeviceIdType.MESH

TOK = 128
D = 768
WID = 192
HEADS = 3
HEAD = 64
CACHE = 32
SRC = 128
ROWS = 32
EXP = 8
CAP = 32


def xor_peer(me, m):
    flip1 = me + 1 - 2 * lax.rem(me, 2)
    if m == 1:
        return flip1
    if m == 2:
        return lax.rem(me + 2, 4)
    return 3 - me


def rms(h_float, scale):
    inv_rms = lax.rsqrt(jnp.mean(h_float * h_float, axis=-1, keepdims=True) + EPS)
    return (h_float * inv_rms * scale).astype(BF16)


def dot(a, b, dims):
    return lax.dot_general(a, b, (dims, ((), ())), preferred_element_type=F32)


NN = ((1,), (0,))
NT = ((1,), (1,))


def kernel(bias_ref, hid_ref, pos_ref, exp_ref, mask_ref, scale_ref, router_ref,
           kc, vc, ck, cv, wq, wk, wv, wo, wcq, wco, wdg, wdu, wdd, weg, weu, wed,
           h_out, kc_out, vc_out,
           kb, vb, ckb, cvb, wqkv, wob, wcqb, wcob, dgb, dub, ddb, egb, eub, edb,
           biasb, sb, q32, ctxb, hown, part, rsb, xb, disp, dispt, recv, eout, ret, gatec,
           in_sem, out_sem, rs_s, rs_r, ag_s, ag_r, a_s, a_r, b_s, b_r):
    me = lax.axis_index("tp")
    ep = lax.axis_index("ep")
    barrier = pltpu.get_barrier_semaphore()
    for m in (1, 2, 3):
        pl.semaphore_signal(barrier, inc=1, device_id={"tp": xor_peer(me, m)}, device_id_type=MESH)
        pl.semaphore_signal(barrier, inc=1, device_id={"ep": xor_peer(ep, m)}, device_id_type=MESH)

    loads = {}

    def load(key, src, dst):
        copy = pltpu.make_async_copy(src, dst, in_sem.at[len(loads)])
        copy.start()
        loads[key] = copy

    def need(*keys):
        for key in keys:
            loads[key].wait()

    def load_self(layer):
        load(f"q{layer}", wq.at[layer], wqkv.at[layer, pl.ds(0, WID)])
        load(f"k{layer}", wk.at[layer], wqkv.at[layer, pl.ds(WID, WID)])
        load(f"v{layer}", wv.at[layer], wqkv.at[layer, pl.ds(2 * WID, WID)])
        load(f"kc{layer}", kc.at[layer], kb.at[layer])
        load(f"vc{layer}", vc.at[layer], vb.at[layer])
        load(f"o{layer}", wo.at[layer], wob.at[layer])

    def load_cross(layer):
        load(f"cq{layer}", wcq.at[layer], wcqb.at[layer])
        load(f"ck{layer}", ck.at[layer], ckb.at[layer])
        load(f"cv{layer}", cv.at[layer], cvb.at[layer])
        load(f"co{layer}", wco.at[layer], wcob.at[layer])

    load_self(0)

    sends = []

    def rs_start(ph, value):
        part[ph] = value.astype(BF16)
        copies = []
        for m in (3, 2, 1):
            peer = xor_peer(me, m)
            copy = pltpu.make_async_remote_copy(
                src_ref=part.at[ph, pl.ds(pl.multiple_of(peer * ROWS, ROWS), ROWS)],
                dst_ref=rsb.at[ph, m - 1],
                send_sem=rs_s.at[ph, m - 1], recv_sem=rs_r.at[ph, m - 1],
                device_id={"tp": peer}, device_id_type=MESH)
            copy.start()
            copies.append(copy)
        sends.extend(copies)
        return copies

    def rs_finish(ph, copies):
        total = part[ph, pl.ds(pl.multiple_of(me * ROWS, ROWS), ROWS), :].astype(F32)
        for copy, m in zip(copies[::-1], (1, 2, 3)):
            copy.wait_recv()
            total = total + rsb[ph, m - 1].astype(F32)
        return total.astype(BF16).astype(F32)

    def gather(ph, own):
        mine = pl.ds(pl.multiple_of(me * ROWS, ROWS), ROWS)
        xb[ph, mine, :] = own
        copies = []
        for m in (3, 2, 1):
            copy = pltpu.make_async_remote_copy(
                src_ref=xb.at[ph, mine], dst_ref=xb.at[ph, mine],
                send_sem=ag_s.at[ph, m - 1], recv_sem=ag_r.at[ph, m - 1],
                device_id={"tp": xor_peer(me, m)}, device_id_type=MESH)
            copy.start()
            copies.append(copy)
        sends.extend(copies)
        for copy in copies[::-1]:
            copy.wait_recv()
        return xb[ph]

    def add_own(delta):
        new = (hown[...] + delta).astype(BF16).astype(F32)
        hown[...] = new
        return new

    pos = pos_ref[...]
    slot_id = lax.broadcasted_iota(jnp.int32, (CACHE, TOK), 0)
    dist = pos - slot_id
    for h in range(HEADS):
        acc = jnp.full((CACHE, TOK), NEG_BIG, F32)
        for d in range(CACHE):
            acc = jnp.where(dist == d, bias_ref[h, d], acc)
        biasb[h] = acc

    def self_attn(layer, x):
        need(f"q{layer}", f"k{layer}", f"v{layer}")
        qkv = dot(wqkv[layer], x, NT).astype(BF16).astype(F32)
        at_slot = dist == 0
        valid = dist >= 0
        need(f"kc{layer}")
        probs = []
        for h in range(HEADS):
            q = qkv[h * HEAD:(h + 1) * HEAD]
            k_new = qkv[WID + h * HEAD:WID + (h + 1) * HEAD]
            for g in range(CACHE // 8):
                kf = kb[layer, h, g * 8:(g + 1) * 8].astype(F32)
                sb[h, g * 8:(g + 1) * 8] = jnp.sum(kf * q[None], axis=1)
            s_new = jnp.sum(q * k_new, axis=0, keepdims=True)
            s = jnp.where(at_slot, s_new, sb[h])
            s = jnp.where(valid, s + biasb[h], NEG_BIG)
            e = jnp.exp(s - jnp.max(s, axis=0, keepdims=True))
            p = e / jnp.sum(e, axis=0, keepdims=True)
            probs.append(p.astype(BF16).astype(F32))
        need(f"vc{layer}")
        outs = []
        for h in range(HEADS):
            v_new = qkv[2 * WID + h * HEAD:2 * WID + (h + 1) * HEAD]
            p_new = jnp.sum(jnp.where(at_slot, probs[h], 0.0), axis=0, keepdims=True)
            sb[h] = jnp.where(at_slot, 0.0, probs[h])
            acc = p_new * v_new
            for j in range(CACHE):
                acc = acc + sb[h, j:j + 1] * vb[layer, h, j].astype(F32)
            outs.append(acc)
        ctx = jnp.concatenate(outs, axis=0).T.astype(BF16)
        need(f"o{layer}")
        return dot(ctx, wob[layer], NN), qkv

    def update_cache(layer, qkv):
        for buf, out, base, key in ((kb, kc_out, WID, 0), (vb, vc_out, 2 * WID, 1)):
            for h in range(HEADS):
                new = qkv[base + h * HEAD:base + (h + 1) * HEAD]
                for j in range(CACHE):
                    buf[layer, h, j] = jnp.where(pos == j, new, buf[layer, h, j].astype(F32)).astype(BF16)
            pltpu.make_async_copy(buf.at[layer], out.at[layer], out_sem.at[layer, key]).start()

    head_row = lax.broadcasted_iota(jnp.int32, (8, WID), 0)
    head_col = lax.broadcasted_iota(jnp.int32, (8, WID), 1)
    low = head_row * HEAD
    head_mask = jnp.where((head_col >= low) & (head_col < low + HEAD), 1.0, 0.0)
    GRP = 16

    def cross_attn(layer, x):
        need(f"cq{layer}")
        q32[...] = dot(x, wcqb[layer], NT).astype(BF16).astype(F32)
        need(f"ck{layer}", f"cv{layer}")

        def group(g, carry):
            base = pl.multiple_of(g * GRP, GRP)
            scores = []
            rows = []
            q_grp = q32[pl.ds(base, GRP), :]
            m_grp = mask_ref[pl.ds(base, GRP), :]
            for i in range(GRP):
                qrow = jnp.broadcast_to(q_grp[i:i + 1], (8, WID))
                qbd = (qrow * head_mask).astype(BF16)
                s = dot(qbd, ckb[layer, base + i], NN)
                m = jnp.broadcast_to(m_grp[i:i + 1], (8, SRC))
                scores.append(jnp.where(m > 0, s, NEG_BIG))
            s = jnp.concatenate(scores, axis=0)
            e = jnp.exp(s - jnp.max(s, axis=-1, keepdims=True))
            p = e / jnp.sum(e, axis=-1, keepdims=True)
            for i in range(GRP):
                c = dot(p[i * 8:(i + 1) * 8].astype(BF16), cvb[layer, base + i], NT)
                rows.append(jnp.sum(c * head_mask, axis=0, keepdims=True))
            ctxb[pl.ds(base, GRP), :] = jnp.concatenate(rows, axis=0)
            return carry

        lax.fori_loop(0, TOK // GRP, group, 0)
        need(f"co{layer}")
        return dot(ctxb[...].astype(BF16), wcob[layer], NN)

    def glu(x, w_gate, w_up):
        return (jax.nn.gelu(dot(x, w_gate, NN)) * dot(x, w_up, NN)).astype(BF16)

    mine = pl.ds(pl.multiple_of(me * ROWS, ROWS), ROWS)
    hown[...] = hid_ref[mine, :].astype(F32)
    x = rms(hid_ref[...].astype(F32), scale_ref[0, 0:1, :])

    for layer in range(2):
        ph = 3 * layer
        partial, qkv = self_attn(layer, x)
        if layer == 0:
            pl.semaphore_wait(barrier, 6)
        copies = rs_start(ph, partial)
        if layer == 0:
            load_cross(0)
            load("dg", wdg, dgb)
            load("du", wdu, dub)
            load("dd", wdd, ddb)
            load_self(1)
            load_cross(1)
            load("eg", weg, egb)
            load("eu", weu, eub)
            load("ed", wed, edb)
        update_cache(layer, qkv)
        new = add_own(rs_finish(ph, copies))
        x = gather(ph, rms(new, scale_ref[1, layer:layer + 1, :]))
        copies = rs_start(ph + 1, cross_attn(layer, x))
        new = add_own(rs_finish(ph + 1, copies))
        x = gather(ph + 1, rms(new, scale_ref[2, layer:layer + 1, :]))
        if layer == 0:
            need("dg", "du", "dd")
            copies = rs_start(2, dot(glu(x, dgb[...], dub[...]), ddb[...], NN))
            new = add_own(rs_finish(2, copies))
            x = gather(2, rms(new, scale_ref[0, 1:2, :]))

    expert = exp_ref[...]
    onehot = jnp.where(lax.broadcasted_iota(jnp.int32, (EXP, TOK), 0) == expert, 1.0, 0.0)
    r_id = lax.broadcasted_iota(jnp.int32, (TOK, TOK), 0)
    c_id = lax.broadcasted_iota(jnp.int32, (TOK, TOK), 1)
    before = jnp.where(r_id < c_id, 1.0, 0.0).astype(BF16)
    count = dot(onehot.astype(BF16), before, NN)
    slot = jnp.sum(count * onehot, axis=0, keepdims=True)
    target = jnp.where(slot < CAP, expert.astype(F32) * CAP + slot, -1.0)
    place = jnp.where(lax.broadcasted_iota(jnp.int32, (EXP * CAP, TOK), 0).astype(F32) == target, 1.0, 0.0)
    disp[...] = dot(place.astype(BF16), x, NN).astype(BF16)

    two = 2 * CAP

    def ep_rows(e):
        return pl.ds(pl.multiple_of(e * two, two), two)

    copies = []
    for m in (3, 2, 1):
        peer = xor_peer(ep, m)
        copy = pltpu.make_async_remote_copy(
            src_ref=disp.at[ep_rows(peer)], dst_ref=recv.at[m],
            send_sem=a_s.at[m - 1], recv_sem=a_r.at[m - 1],
            device_id={"ep": peer}, device_id_type=MESH)
        copy.start()
        copies.append(copy)
    sends.extend(copies)
    recv[0] = disp[ep_rows(ep), :]
    dispt[...] = place.T.astype(BF16)

    logits = lax.dot_general(router_ref[...], x.astype(F32), (NT, ((), ())), precision=lax.Precision.HIGHEST,
                             preferred_element_type=F32)
    e = jnp.exp(logits - jnp.max(logits, axis=0, keepdims=True))
    route = e / jnp.sum(e, axis=0, keepdims=True)
    gate_row = jnp.sum(route * onehot, axis=0, keepdims=True)
    gatec[...] = jnp.broadcast_to(gate_row, (TOK, TOK)).T

    need("eg", "eu", "ed")
    for copy in copies:
        copy.wait_recv()
    for j in range(2):
        rows = recv[:, j * CAP:(j + 1) * CAP, :].reshape(4 * CAP, D)
        out = dot(glu(rows, egb[j], eub[j]), edb[j], NN).astype(BF16)
        eout[:, j * CAP:(j + 1) * CAP, :] = out.reshape(4, CAP, D)
    copies = []
    for m in (3, 2, 1):
        peer = xor_peer(ep, m)
        copy = pltpu.make_async_remote_copy(
            src_ref=eout.at[m], dst_ref=ret.at[ep_rows(ep)],
            send_sem=b_s.at[m - 1], recv_sem=b_r.at[m - 1],
            device_id={"ep": peer}, device_id_type=MESH)
        copy.start()
        copies.append(copy)
    sends.extend(copies)
    ret[ep_rows(ep), :] = eout[0]
    for copy in copies:
        copy.wait_recv()
    copies = rs_start(5, dot(dispt[...], ret[...], NN))
    y = rs_finish(5, copies)
    gate_own = gatec[mine, :][:, 0:1]
    new = (hown[...] + gate_own * y).astype(BF16)
    h_out[...] = gather(5, new)

    for copy in sends:
        copy.wait_send()
    for layer in range(2):
        pltpu.make_async_copy(kb.at[layer], kc_out.at[layer], out_sem.at[layer, 0]).wait()
        pltpu.make_async_copy(vb.at[layer], vc_out.at[layer], out_sem.at[layer, 1]).wait()


def decode_body(hidden, write_pos, enc_mask, expert_idx, self_keys, self_values, cross_keys, cross_values, rel_bias, norm_scale, w_query, w_key, w_value, w_out, w_cross_query, w_cross_out, dense_gate, dense_up, dense_down, router, exp_gate, exp_up, exp_down):
    k_t = jnp.transpose(self_keys, (0, 2, 3, 4, 1))
    v_t = jnp.transpose(self_values, (0, 2, 3, 4, 1))
    ck_t = jnp.transpose(cross_keys, (0, 1, 2, 4, 3)).reshape(2, TOK, WID, SRC)
    cv_t = jnp.transpose(cross_values, (0, 1, 2, 4, 3)).reshape(2, TOK, WID, SRC)
    swap = lambda w: jnp.transpose(w, (0, 2, 1))
    vmem = pl.BlockSpec(memory_space=pltpu.VMEM)
    hbm = pl.BlockSpec(memory_space=pl.ANY)
    smem = pl.BlockSpec(memory_space=pltpu.SMEM)
    cache = (2, HEADS, CACHE, HEAD, TOK)
    dma = pltpu.SemaphoreType.DMA
    h_new, k_new, v_new = pl.pallas_call(
        kernel,
        out_shape=(jax.ShapeDtypeStruct((TOK, D), BF16), jax.ShapeDtypeStruct(cache, BF16), jax.ShapeDtypeStruct(cache, BF16)),
        in_specs=[smem] + [vmem] * 6 + [hbm] * 16,
        out_specs=(vmem, hbm, hbm),
        scratch_shapes=[
            pltpu.VMEM(cache, BF16), pltpu.VMEM(cache, BF16),
            pltpu.VMEM((2, TOK, WID, SRC), BF16), pltpu.VMEM((2, TOK, WID, SRC), BF16),
            pltpu.VMEM((2, 3 * WID, D), BF16), pltpu.VMEM((2, WID, D), BF16),
            pltpu.VMEM((2, WID, D), BF16), pltpu.VMEM((2, WID, D), BF16),
            pltpu.VMEM((D, D), BF16), pltpu.VMEM((D, D), BF16), pltpu.VMEM((D, D), BF16),
            pltpu.VMEM((2, D, D), BF16), pltpu.VMEM((2, D, D), BF16), pltpu.VMEM((2, D, D), BF16),
            pltpu.VMEM((HEADS, CACHE, TOK), F32), pltpu.VMEM((HEADS, CACHE, TOK), F32),
            pltpu.VMEM((TOK, WID), F32), pltpu.VMEM((TOK, WID), F32), pltpu.VMEM((ROWS, D), F32),
            pltpu.VMEM((6, TOK, D), BF16), pltpu.VMEM((6, 3, ROWS, D), BF16), pltpu.VMEM((6, TOK, D), BF16),
            pltpu.VMEM((EXP * CAP, D), BF16), pltpu.VMEM((TOK, EXP * CAP), BF16),
            pltpu.VMEM((4, 2 * CAP, D), BF16), pltpu.VMEM((4, 2 * CAP, D), BF16), pltpu.VMEM((EXP * CAP, D), BF16),
            pltpu.VMEM((TOK, TOK), F32),
            dma((32,)), dma((2, 2)), dma((6, 3)), dma((6, 3)), dma((6, 3)), dma((6, 3)),
            dma((3,)), dma((3,)), dma((3,)), dma((3,)),
        ],
        compiler_params=pltpu.CompilerParams(collective_id=0, has_side_effects=True, vmem_limit_bytes=63 << 20),
        name="decode",
    )(rel_bias, hidden, write_pos.reshape(1, TOK), expert_idx.reshape(1, TOK), enc_mask, jnp.transpose(norm_scale, (1, 0, 2)), router.T,
      k_t, v_t, ck_t, cv_t, swap(w_query), swap(w_key), swap(w_value), w_out, swap(w_cross_query), w_cross_out,
      dense_gate, dense_up, dense_down, exp_gate, exp_up, exp_down)
    back = lambda c: jnp.transpose(c, (0, 4, 1, 2, 3))
    return h_new, back(k_new), back(v_new)


def solution(mesh):
    batch = ('dp', 'ep')
    row_spec = P(batch, None)
    vec_spec = P(batch)
    cache_spec = P(None, batch, 'tp', None, None)
    col_spec = P(None, None, 'tp')
    out_rows = P(None, 'tp', None)
    in_specs = (row_spec, vec_spec, row_spec, vec_spec, cache_spec, cache_spec, cache_spec, cache_spec, P('tp', None), P(), col_spec, col_spec, col_spec, out_rows, col_spec, out_rows, P(None, 'tp'), P(None, 'tp'), P('tp', None), P(), P('ep', None, 'tp'), P('ep', None, 'tp'), P('ep', 'tp', None))
    out_specs = (row_spec, cache_spec, cache_spec)
    return jax.shard_map(decode_body, mesh=mesh, in_specs=in_specs, out_specs=out_specs, check_vma=False)
```

```python
import functools

import jax
import jax.numpy as jnp
from jax import lax
from jax.experimental import pallas as pl
from jax.experimental.pallas import tpu as pltpu
from jax.sharding import PartitionSpec as P

EPS = 1e-6
NEG_BIG = -1e9
F32 = jnp.float32
BF16 = jnp.bfloat16
MESH = pl.DeviceIdType.MESH

TOK = 128
D = 768
WID = 192
HEADS = 3
HEAD = 64
CACHE = 32
SRC = 128
HALF = 64
ROWS = 16
GRP = 16
VMEM_LIMIT = 55 << 20
EXP = 8
CAP = 32


def xor_peer(me, m):
    flip1 = me + 1 - 2 * lax.rem(me, 2)
    if m == 1:
        return flip1
    if m == 2:
        return lax.rem(me + 2, 4)
    return 3 - me


def rms(h_float, scale):
    inv_rms = lax.rsqrt(jnp.mean(h_float * h_float, axis=-1, keepdims=True) + EPS)
    return (h_float * inv_rms * scale).astype(BF16)


def dot(a, b, dims):
    return lax.dot_general(a, b, (dims, ((), ())), preferred_element_type=F32)


NN = ((1,), (0,))
NT = ((1,), (1,))


def kernel(bias_h, hid_h, pos_h, exp_h, mask_h, scale_h, router_h,
           kc, vc, ck, cv, wq, wk, wv, wo, wcq, wco, wdg, wdu, wdd, weg, weu, wed,
           h_out, kb, vb,
           bias_ref, hid_ref, pos_ref, exp_ref, mask_ref, scale_ref, router_ref,
           ckb, cvb, wqkv, wob, wcqb, wcob, dgb, dub, ddb, egb, eub, edb,
           biasb, sb, sc, pb, ctxb, part, rsb, hb, disp, dispt, recv, eout, ret, gatec,
           in_sem, rs_s, rs_r, ag_s, ag_r, a_s, a_r, b_s, b_r):
    me = lax.axis_index("tp")
    ep = lax.axis_index("ep")
    barrier = pltpu.get_barrier_semaphore()
    for m in (1, 2, 3):
        pl.semaphore_signal(barrier, inc=1, device_id={"tp": xor_peer(me, m)}, device_id_type=MESH)
        pl.semaphore_signal(barrier, inc=1, device_id={"ep": xor_peer(ep, m)}, device_id_type=MESH)

    loads = {}

    def load(key, src, dst):
        copy = pltpu.make_async_copy(src, dst, in_sem.at[len(loads)])
        copy.start()
        loads[key] = copy

    def need(*keys):
        for key in keys:
            loads[key].wait()

    def load_self(layer):
        load(f"q{layer}", wq.at[layer], wqkv.at[layer, pl.ds(0, WID)])
        load(f"k{layer}", wk.at[layer], wqkv.at[layer, pl.ds(WID, WID)])
        load(f"v{layer}", wv.at[layer], wqkv.at[layer, pl.ds(2 * WID, WID)])
        load(f"kc{layer}", kc.at[layer], kb.at[layer])
        load(f"vc{layer}", vc.at[layer], vb.at[layer])
        load(f"o{layer}", wo.at[layer], wob.at[layer])

    def load_cross(layer):
        load(f"cq{layer}", wcq.at[layer], wcqb.at[layer])
        load(f"ck{layer}", ck.at[layer], ckb.at[layer])
        load(f"cv{layer}", cv.at[layer], cvb.at[layer])
        load(f"co{layer}", wco.at[layer], wcob.at[layer])

    load("hid", hid_h, hid_ref)
    load("scale", scale_h, scale_ref)
    load("pos", pos_h, pos_ref)
    load("bias", bias_h, bias_ref)
    load_self(0)
    load("exp", exp_h, exp_ref)
    load("mask", mask_h, mask_ref)
    load("router", router_h, router_ref)

    def load_rest():
        load_cross(0)
        load("dg", wdg, dgb)
        load("du", wdu, dub)
        load("dd", wdd, ddb)
        load_self(1)
        load_cross(1)
        load("eg", weg, egb)
        load("eu", weu, eub)
        load("ed", wed, edb)

    sends = []
    pending = {}

    def block(p, owner):
        return pl.ds(pl.multiple_of(p * HALF + owner * ROWS, ROWS), ROWS)

    def rs_start(ph, p, value):
        part[ph, p * HALF:(p + 1) * HALF] = value.astype(BF16)
        for m in (3, 2, 1):
            peer = xor_peer(me, m)
            copy = pltpu.make_async_remote_copy(
                src_ref=part.at[ph, block(p, peer)], dst_ref=rsb.at[ph, p, m - 1],
                send_sem=rs_s.at[ph, p, m - 1], recv_sem=rs_r.at[ph, p, m - 1],
                device_id={"tp": peer}, device_id_type=MESH)
            copy.start()
            sends.append(copy)
            pending[ph, p, m] = copy

    def rs_finish(ph, p):
        total = part[ph, block(p, me), :].astype(F32)
        for m in (1, 2, 3):
            pending[ph, p, m].wait_recv()
            total = total + rsb[ph, p, m - 1].astype(F32)
        return total.astype(BF16).astype(F32)

    def gather_start(ph, p, own):
        mine = block(p, me)
        hb[ph, mine, :] = own
        for m in (3, 2, 1):
            copy = pltpu.make_async_remote_copy(
                src_ref=hb.at[ph, mine], dst_ref=hb.at[ph, mine],
                send_sem=ag_s.at[ph, p, m - 1], recv_sem=ag_r.at[ph, p, m - 1],
                device_id={"tp": xor_peer(me, m)}, device_id_type=MESH)
            copy.start()
            sends.append(copy)
            pending["g", ph, p, m] = copy

    def gather_wait(ph, p):
        for m in (1, 2, 3):
            pending["g", ph, p, m].wait_recv()
        return hb[ph, p * HALF:(p + 1) * HALF]

    def reduce_gather(ph, before):
        for p in (0, 1):
            own = before[block(p, me), :].astype(F32)
            gather_start(ph, p, (own + rs_finish(ph, p)).astype(BF16))

    def self_attn(layer, x):
        need(f"q{layer}", f"k{layer}", f"v{layer}")
        pos = pos_ref[...]
        dist = pos - lax.broadcasted_iota(jnp.int32, (CACHE, TOK), 0)
        at_slot = dist == 0
        valid = dist >= 0
        qkv = dot(wqkv[layer], x, NT).astype(BF16).astype(F32)
        if layer == 0:
            need("bias")
            for h in range(HEADS):
                acc = jnp.full((CACHE, TOK), NEG_BIG, F32)
                for d in range(CACHE):
                    acc = jnp.where(dist == d, bias_ref[h, d], acc)
                biasb[h] = acc
        need(f"kc{layer}")
        probs = []
        for h in range(HEADS):
            q = qkv[h * HEAD:(h + 1) * HEAD]
            k_new = qkv[WID + h * HEAD:WID + (h + 1) * HEAD]
            for g in range(CACHE // 8):
                kf = kb[layer, h, g * 8:(g + 1) * 8].astype(F32)
                sb[h, g * 8:(g + 1) * 8] = jnp.sum(kf * q[None], axis=1)
            s_new = jnp.sum(q * k_new, axis=0, keepdims=True)
            s = jnp.where(at_slot, s_new, sb[h])
            s = jnp.where(valid, s + biasb[h], NEG_BIG)
            e = jnp.exp(s - jnp.max(s, axis=0, keepdims=True))
            p = e / jnp.sum(e, axis=0, keepdims=True)
            probs.append(p.astype(BF16).astype(F32))
        need(f"vc{layer}")
        if layer == 0:
            load_rest()
        outs = []
        for h in range(HEADS):
            v_new = qkv[2 * WID + h * HEAD:2 * WID + (h + 1) * HEAD]
            p_new = jnp.sum(jnp.where(at_slot, probs[h], 0.0), axis=0, keepdims=True)
            sb[h] = jnp.where(at_slot, 0.0, probs[h])
            acc = p_new * v_new
            for j in range(CACHE):
                acc = acc + sb[h, j:j + 1] * vb[layer, h, j].astype(F32)
            outs.append(acc)
        ctx = jnp.concatenate(outs, axis=0).T.astype(BF16)
        need(f"o{layer}")
        partial = dot(ctx, wob[layer], NN)
        if layer == 0:
            pl.semaphore_wait(barrier, 6)
        for p in (0, 1):
            rs_start(3 * layer, p, partial[p * HALF:(p + 1) * HALF])
        for buf, base in ((kb, WID), (vb, 2 * WID)):
            for h in range(HEADS):
                new = qkv[base + h * HEAD:base + (h + 1) * HEAD]
                for j in range(CACHE):
                    buf[layer, h, j] = jnp.where(pos == j, new, buf[layer, h, j].astype(F32)).astype(BF16)

    head_row = lax.broadcasted_iota(jnp.int32, (8, WID), 0)
    head_col = lax.broadcasted_iota(jnp.int32, (8, WID), 1)
    low = head_row * HEAD
    head_mask = jnp.where((head_col >= low) & (head_col < low + HEAD), 1.0, 0.0)
    lane = lax.broadcasted_iota(jnp.int32, (HEAD, GRP * 8), 1)

    def cross_attn(layer, p, x):
        q = dot(x, wcqb[layer], NT).astype(BF16).astype(F32)
        for i in range(HALF):
            t = p * HALF + i
            qbd = (jnp.broadcast_to(q[i:i + 1], (8, WID)) * head_mask).astype(BF16)
            s = dot(qbd, ckb[layer, t], NN)
            m = jnp.broadcast_to(mask_ref[t:t + 1, :], (8, SRC))
            sc[i * 8:(i + 1) * 8] = jnp.where(m > 0, s, NEG_BIG)
        for g in range(HALF // GRP):
            s = sc[g * GRP * 8:(g + 1) * GRP * 8]
            e = jnp.exp(s - jnp.max(s, axis=-1, keepdims=True))
            pb[g * GRP * 8:(g + 1) * GRP * 8] = (e / jnp.sum(e, axis=-1, keepdims=True)).astype(BF16)
        for g in range(HALF // GRP):
            prob = pb[g * GRP * 8:(g + 1) * GRP * 8]
            acc = [jnp.zeros((HEAD, GRP * 8), F32)] * HEADS
            for i in range(GRP):
                c = dot(cvb[layer, p * HALF + g * GRP + i], prob, NT)
                for h in range(HEADS):
                    acc[h] = jnp.where(lane == i * 8 + h, c[h * HEAD:(h + 1) * HEAD], acc[h])
            rows = jnp.concatenate(acc, axis=0).T
            ctxb[g * GRP:(g + 1) * GRP, :] = jnp.sum(rows.reshape(GRP, 8, WID), axis=1)
        return dot(ctxb[...].astype(BF16), wcob[layer], NN)

    def glu(x, w_gate, w_up):
        return (jax.nn.gelu(dot(x, w_gate, NN)) * dot(x, w_up, NN)).astype(BF16)

    need("hid", "scale", "pos")
    x = rms(hid_ref[...].astype(F32), scale_ref[0, 0:1, :])

    for layer in range(2):
        ph = 3 * layer
        self_attn(layer, x)
        reduce_gather(ph, hid_ref if layer == 0 else hb.at[2])
        need(f"cq{layer}", f"ck{layer}", f"cv{layer}", f"co{layer}")
        if layer == 0:
            need("mask")
        for p in (0, 1):
            x = rms(gather_wait(ph, p).astype(F32), scale_ref[1, layer:layer + 1, :])
            rs_start(ph + 1, p, cross_attn(layer, p, x))
        reduce_gather(ph + 1, hb.at[ph])
        if layer == 0:
            need("dg", "du", "dd")
            for p in (0, 1):
                x = rms(gather_wait(1, p).astype(F32), scale_ref[2, 0:1, :])
                rs_start(2, p, dot(glu(x, dgb[...], dub[...]), ddb[...], NN))
            reduce_gather(2, hb.at[1])
            x = jnp.concatenate([rms(gather_wait(2, p).astype(F32), scale_ref[0, 1:2, :]) for p in (0, 1)], axis=0)

    need("exp", "router")
    expert = exp_ref[...]
    onehot = jnp.where(lax.broadcasted_iota(jnp.int32, (EXP, TOK), 0) == expert, 1.0, 0.0)
    r_id = lax.broadcasted_iota(jnp.int32, (TOK, TOK), 0)
    c_id = lax.broadcasted_iota(jnp.int32, (TOK, TOK), 1)
    before = jnp.where(r_id < c_id, 1.0, 0.0).astype(BF16)
    count = dot(onehot.astype(BF16), before, NN)
    slot = jnp.sum(count * onehot, axis=0, keepdims=True)
    target = jnp.where(slot < CAP, expert.astype(F32) * CAP + slot, -1.0)
    place = jnp.where(lax.broadcasted_iota(jnp.int32, (EXP * CAP, TOK), 0).astype(F32) == target, 1.0, 0.0)
    dispt[...] = place.T.astype(BF16)
    x = jnp.concatenate([rms(gather_wait(4, p).astype(F32), scale_ref[2, 1:2, :]) for p in (0, 1)], axis=0)
    disp[...] = dot(place.astype(BF16), x, NN).astype(BF16)

    def ep_rows(e, j):
        return pl.ds(pl.multiple_of((2 * e + j) * CAP, CAP), CAP)

    for j in (0, 1):
        for m in (3, 2, 1):
            peer = xor_peer(ep, m)
            copy = pltpu.make_async_remote_copy(
                src_ref=disp.at[ep_rows(peer, j)], dst_ref=recv.at[j, m],
                send_sem=a_s.at[j, m - 1], recv_sem=a_r.at[j, m - 1],
                device_id={"ep": peer}, device_id_type=MESH)
            copy.start()
            sends.append(copy)
            pending["a", j, m] = copy
    for j in (0, 1):
        recv[j, 0] = disp[ep_rows(ep, j), :]

    logits = lax.dot_general(router_ref[...], x.astype(F32), (NT, ((), ())), precision=lax.Precision.HIGHEST,
                             preferred_element_type=F32)
    e = jnp.exp(logits - jnp.max(logits, axis=0, keepdims=True))
    route = e / jnp.sum(e, axis=0, keepdims=True)
    gate_row = jnp.sum(route * onehot, axis=0, keepdims=True)
    gatec[...] = jnp.broadcast_to(gate_row, (TOK, TOK)).T

    need("eg", "eu", "ed")
    for j in (0, 1):
        for m in (1, 2, 3):
            pending["a", j, m].wait_recv()
        rows = recv[j].reshape(4 * CAP, D)
        eout[j] = dot(glu(rows, egb[j], eub[j]), edb[j], NN).astype(BF16).reshape(4, CAP, D)
        for m in (3, 2, 1):
            peer = xor_peer(ep, m)
            copy = pltpu.make_async_remote_copy(
                src_ref=eout.at[j, m], dst_ref=ret.at[ep_rows(ep, j)],
                send_sem=b_s.at[j, m - 1], recv_sem=b_r.at[j, m - 1],
                device_id={"ep": peer}, device_id_type=MESH)
            copy.start()
            sends.append(copy)
            pending["b", j, m] = copy
        ret[ep_rows(ep, j), :] = eout[j, 0]
    for j in (0, 1):
        for m in (1, 2, 3):
            pending["b", j, m].wait_recv()
    for p in (0, 1):
        rs_start(5, p, dot(dispt[p * HALF:(p + 1) * HALF], ret[...], NN))
    for p in (0, 1):
        y = rs_finish(5, p)
        mine = block(p, me)
        gather_start(5, p, (hb[4, mine, :].astype(F32) + gatec[mine, :][:, 0:1] * y).astype(BF16))
    for p in (0, 1):
        h_out[p * HALF:(p + 1) * HALF] = gather_wait(5, p)
    for copy in sends:
        copy.wait_send()


def store(h_v, k_v, v_v, h_o, k_o, v_o, sem):
    copies = [pltpu.make_async_copy(src, dst, sem.at[i]) for i, (src, dst) in enumerate(((k_v, k_o), (v_v, v_o), (h_v, h_o)))]
    for copy in copies:
        copy.start()
    for copy in copies:
        copy.wait()


def decode_body(hidden, write_pos, enc_mask, expert_idx, self_keys, self_values, cross_keys, cross_values, rel_bias, norm_scale, w_query, w_key, w_value, w_out, w_cross_query, w_cross_out, dense_gate, dense_up, dense_down, router, exp_gate, exp_up, exp_down):
    k_t = jnp.transpose(self_keys, (0, 2, 3, 4, 1))
    v_t = jnp.transpose(self_values, (0, 2, 3, 4, 1))
    ck_t = jnp.transpose(cross_keys, (0, 1, 2, 4, 3)).reshape(2, TOK, WID, SRC)
    cv_t = jnp.transpose(cross_values, (0, 1, 2, 4, 3)).reshape(2, TOK, WID, SRC)
    swap = lambda w: jnp.transpose(w, (0, 2, 1))
    vmem = pl.BlockSpec(memory_space=pltpu.VMEM)
    hbm = pl.BlockSpec(memory_space=pl.ANY)
    cache = (2, HEADS, CACHE, HEAD, TOK)
    dma = pltpu.SemaphoreType.DMA
    out_shape = (jax.ShapeDtypeStruct((TOK, D), BF16), jax.ShapeDtypeStruct(cache, BF16), jax.ShapeDtypeStruct(cache, BF16))
    outs = pl.pallas_call(
        kernel,
        out_shape=tuple(pltpu.VMEM(o.shape, o.dtype) for o in out_shape),
        in_specs=[hbm] * 23,
        out_specs=(vmem, vmem, vmem),
        scratch_shapes=[
            pltpu.SMEM((HEADS, CACHE), F32), pltpu.VMEM((TOK, D), BF16), pltpu.VMEM((1, TOK), jnp.int32), pltpu.VMEM((1, TOK), jnp.int32),
            pltpu.VMEM((TOK, SRC), jnp.int32), pltpu.VMEM((3, 2, D), F32), pltpu.VMEM((EXP, D), F32),
            pltpu.VMEM((2, TOK, WID, SRC), BF16), pltpu.VMEM((2, TOK, WID, SRC), BF16),
            pltpu.VMEM((2, 3 * WID, D), BF16), pltpu.VMEM((2, WID, D), BF16),
            pltpu.VMEM((2, WID, D), BF16), pltpu.VMEM((2, WID, D), BF16),
            pltpu.VMEM((D, D), BF16), pltpu.VMEM((D, D), BF16), pltpu.VMEM((D, D), BF16),
            pltpu.VMEM((2, D, D), BF16), pltpu.VMEM((2, D, D), BF16), pltpu.VMEM((2, D, D), BF16),
            pltpu.VMEM((HEADS, CACHE, TOK), F32), pltpu.VMEM((HEADS, CACHE, TOK), F32),
            pltpu.VMEM((HALF * 8, SRC), F32), pltpu.VMEM((HALF * 8, SRC), BF16), pltpu.VMEM((HALF, WID), F32),
            pltpu.VMEM((6, TOK, D), BF16), pltpu.VMEM((6, 2, 3, ROWS, D), BF16), pltpu.VMEM((6, TOK, D), BF16),
            pltpu.VMEM((EXP * CAP, D), BF16), pltpu.VMEM((TOK, EXP * CAP), BF16),
            pltpu.VMEM((2, 4, CAP, D), BF16), pltpu.VMEM((2, 4, CAP, D), BF16), pltpu.VMEM((EXP * CAP, D), BF16),
            pltpu.VMEM((TOK, TOK), F32),
            dma((40,)), dma((6, 2, 3)), dma((6, 2, 3)), dma((6, 2, 3)), dma((6, 2, 3)),
            dma((2, 3)), dma((2, 3)), dma((2, 3)), dma((2, 3)),
        ],
        compiler_params=pltpu.CompilerParams(collective_id=0, has_side_effects=True, vmem_limit_bytes=VMEM_LIMIT),
        name="decode",
    )(rel_bias, hidden, write_pos.reshape(1, TOK), expert_idx.reshape(1, TOK), enc_mask, jnp.transpose(norm_scale, (1, 0, 2)), router.T,
      k_t, v_t, ck_t, cv_t, swap(w_query), swap(w_key), swap(w_value), w_out, swap(w_cross_query), w_cross_out,
      dense_gate, dense_up, dense_down, exp_gate, exp_up, exp_down)
    h_new, k_new, v_new = pl.pallas_call(
        store, out_shape=out_shape, in_specs=[vmem] * 3, out_specs=(hbm, hbm, hbm),
        scratch_shapes=[dma((3,))], compiler_params=pltpu.CompilerParams(vmem_limit_bytes=1 << 20), name="store")(*outs)
    back = lambda c: jnp.transpose(c, (0, 4, 1, 2, 3))
    return h_new, back(k_new), back(v_new)


def solution(mesh):
    batch = ('dp', 'ep')
    row_spec = P(batch, None)
    vec_spec = P(batch)
    cache_spec = P(None, batch, 'tp', None, None)
    col_spec = P(None, None, 'tp')
    out_rows = P(None, 'tp', None)
    in_specs = (row_spec, vec_spec, row_spec, vec_spec, cache_spec, cache_spec, cache_spec, cache_spec, P('tp', None), P(), col_spec, col_spec, col_spec, out_rows, col_spec, out_rows, P(None, 'tp'), P(None, 'tp'), P('tp', None), P(), P('ep', None, 'tp'), P('ep', None, 'tp'), P('ep', 'tp', None))
    out_specs = (row_spec, cache_spec, cache_spec)
    return jax.shard_map(decode_body, mesh=mesh, in_specs=in_specs, out_specs=out_specs, check_vma=False)
```
